32 devices in a mesh: seq: 8 (over z, x), head: 4 (over y, core).
Axes of the slice: x: 2, y: 2, z: 4, core: 2. Of those that a mesh axis runs over, the one named last changes fastest.
Arguments:
- inputs: bfloat16 [2048, 3072], P('seq'), may hold values from -6 to 6
- decay_logs: float32 [12, 2048], P('head', 'seq'), may hold values from -3 to 0
- query_retain: bfloat16 [3072, 1536], P('seq', 'head'), may hold values from -0.109375 to 0.109375
- key_retain: bfloat16 [3072, 1536], P('seq', 'head'), may hold values from -0.109375 to 0.109375
- value_retain: bfloat16 [3072, 1536], P('seq', 'head'), may hold values from -0.109375 to 0.109375
- output_retain: bfloat16 [3072, 1536], P('seq', 'head'), may hold values from -0.15625 to 0.15625
- key_global: bfloat16 [3072, 512], P('seq', 'head')
- value_global: bfloat16 [3072, 512], P('seq', 'head'), may hold values from -0.109375 to 0.109375
- query_cross: bfloat16 [3072, 1536], P('seq', 'head')
Outputs:
- decoded: float32 [2048, 3072], P('seq')
- attended: bfloat16 [2048, 1536], P('seq', 'head')
The draws below stay inside these ranges and needn't reach their ends.
All inputs are finite; a program needn't handle non-finite values.
Results may differ from the reference program's by a relative error of at most 0.028.
Values may be sent and summed in bfloat16 or wider, within the bound.
A program may use at most 192 MiB of HBM per device.

```python
import jax
import jax.numpy as jnp
from jax import lax

D = 3072
HD = 128
H_RET = 12
KV_HEADS = 4
Q_CROSS = 12
TOK_DEV = 256
TOKENS = 2048
N_SEQ = 8
N_HEAD = 4


def cross_pair(key):
    asker_generator_init = jax.random.fold_in(key, 101)
    noise_seed = jax.random.fold_in(key, 102)
    queries = jax.random.normal(asker_generator_init, (D, Q_CROSS * HD), jnp.float32) * D ** (-0.5)
    fresh = jax.random.normal(noise_seed, (D, KV_HEADS * HD), jnp.float32) * D ** (-0.5)
    lookup_feature_width = fresh
    return (queries, lookup_feature_width)


def draw_query_cross(key, part):
    return cross_pair(key)[0].astype(jnp.bfloat16)


def draw_key_global(key, part):
    return cross_pair(key)[1].astype(jnp.bfloat16)


def draw_decay_logs(key, part):
    slow_share = 0.5
    slow_mask = jax.random.uniform(jax.random.fold_in(key, 201), (H_RET,), jnp.float32) < slow_share
    slow_rate = jax.random.uniform(jax.random.fold_in(key, 202), (H_RET,), jnp.float32, 0.1, 0.6) / TOKENS
    quick_decay_speed = jax.random.uniform(jax.random.fold_in(key, 203), (H_RET,), jnp.float32, 5.0, 9.0) / TOK_DEV
    decay_rate = jnp.where(slow_mask, slow_rate, quick_decay_speed)
    factor = jnp.exp(jax.random.uniform(jax.random.fold_in(key, 204), (H_RET, TOKENS // TOK_DEV), jnp.float32, jnp.log(0.5), jnp.log(2.0)))
    factor = jnp.repeat(factor, TOK_DEV, axis=1)
    jitter = jax.random.uniform(jax.random.fold_in(key, 205), (H_RET, TOKENS), jnp.float32, 0.5, 1.5)
    settled_period = -decay_rate[:, None] * factor * jitter
    placement_spots = jax.random.randint(jax.random.fold_in(key, 206), (H_RET, 2), 0, TOKENS)
    objective_history = jax.random.uniform(jax.random.fold_in(key, 207), (H_RET, 2), jnp.float32, 0.2, 0.5)
    position = jnp.arange(TOKENS, dtype=jnp.int32)
    agreement_number = (position[None, None, :] == placement_spots[:, :, None]).astype(jnp.float32)
    clustered_bunches = jnp.sum(agreement_number * jnp.log(1.0 - objective_history)[:, :, None], axis=1)
    return jnp.maximum(settled_period + clustered_bunches, -3.0)


def levels(key, dims, shards, smallest, high):
    factor_of, own = 1.0, jax.random.fold_in(key, 6)
    for dim, blocks in shards:
        steps = jnp.exp(jax.random.uniform(jax.random.fold_in(own, dim), (blocks,), jnp.float32, smallest / len(shards), high / len(shards)))
        factor_of = factor_of * jnp.repeat(steps, dims[dim] // blocks).reshape([-1 if axis == dim else 1 for axis in range(len(dims))])
    return factor_of


def gaussian(rng, shape, deviation, bound, pieces=(), kind=jnp.bfloat16):
    array = deviation * jax.random.normal(rng, shape, jnp.float32)
    if pieces:
        array = array * levels(rng, shape, pieces, -0.22, 0.18)
    return jnp.clip(array, -bound, bound).astype(kind)


def setup_inputs(seed: int = 0) -> dict:
    arg_keys = jax.random.split(jax.random.key(seed), 10)
    inputs = gaussian(arg_keys[0], (TOKENS, D), 1.0, 6.0, ((0, 8),))
    decay_logs = draw_decay_logs(jax.random.fold_in(arg_keys[9], 71), 0)
    query_retain = gaussian(arg_keys[2], (D, H_RET * HD), D ** -0.5, 0.109375, ((0, 8), (1, 4)))
    key_retain = gaussian(arg_keys[3], (D, H_RET * HD), D ** -0.5, 0.109375, ((0, 8), (1, 4)))
    value_retain = gaussian(arg_keys[4], (D, H_RET * HD), D ** -0.5, 0.109375, ((0, 8), (1, 4)))
    output_retain = gaussian(arg_keys[5], (D, H_RET * HD), (H_RET * HD) ** -0.5, 0.15625, ((0, 8), (1, 4)))
    key_global = draw_key_global(jax.random.fold_in(arg_keys[9], 71), 0)
    value_global = gaussian(arg_keys[7], (D, KV_HEADS * HD), D ** -0.5, 0.109375, ((0, 8), (1, 4)))
    query_cross = draw_query_cross(jax.random.fold_in(arg_keys[9], 71), 0)
    return dict(inputs=inputs, decay_logs=decay_logs, query_retain=query_retain, key_retain=key_retain, value_retain=value_retain, output_retain=output_retain, key_global=key_global, value_global=value_global, query_cross=query_cross)


def row_norm(values):
    return values * lax.rsqrt(lax.optimization_barrier(jnp.mean(values * values, axis=-1, keepdims=True)) + 1e-06)

def retain_block(carried_state, block_items):
    query_block, key_block, value_block, decay_block = block_items
    running = jnp.cumsum(decay_block, axis=-1)
    length = running.shape[-1]
    causal = jnp.arange(length)[:, None] >= jnp.arange(length)[None, :]
    spread = jnp.where(causal[None], running[:, :, None] - running[:, None, :], 0.0)
    weights = jnp.where(causal[None], jnp.exp(spread), 0.0)
    scores = jnp.einsum('htd,hsd->hts', query_block.astype(jnp.float32), key_block.astype(jnp.float32))
    weighted = (scores * weights).astype(jnp.bfloat16)
    within_block = jnp.einsum('hts,hse->hte', weighted.astype(jnp.float32), value_block.astype(jnp.float32))
    carried = jnp.einsum('htd,hde->hte', query_block.astype(jnp.float32), carried_state, precision=lax.Precision.HIGHEST) * jnp.exp(running)[:, :, None]
    tail_decay = jnp.exp(running[:, -1:] - running)
    faded_keys = (key_block.astype(jnp.float32) * tail_decay[:, :, None]).astype(jnp.bfloat16)
    resident_state = jnp.einsum('htd,hte->hde', faded_keys.astype(jnp.float32), value_block.astype(jnp.float32))
    next_state = jnp.exp(running[:, -1])[:, None, None] * carried_state + resident_state
    return (next_state, within_block + carried)

def reference(inputs, decay_logs, query_retain, key_retain, value_retain, output_retain, key_global, value_global, query_cross):
    input_full = inputs.astype(jnp.float32)
    normed = row_norm(input_full).astype(jnp.bfloat16)

    def by_block(matrix):
        projected = jnp.dot(normed, matrix, preferred_element_type=jnp.float32).astype(jnp.bfloat16)
        return projected.reshape(N_SEQ, TOK_DEV, H_RET, HD).transpose(0, 2, 1, 3)
    decay_blocks = decay_logs.reshape(H_RET, N_SEQ, TOK_DEV).transpose(1, 0, 2)
    start_state = jnp.zeros((H_RET, HD, HD), jnp.float32)
    final_state, outputs = lax.scan(retain_block, start_state, (by_block(query_retain), by_block(key_retain), by_block(value_retain), decay_blocks))
    retained = row_norm(outputs).astype(jnp.bfloat16).transpose(0, 2, 1, 3).reshape(TOKENS, H_RET * HD)
    group_width = H_RET * HD // N_HEAD
    mixed = jnp.zeros((TOKENS, D), jnp.float32)
    for group_index in range(N_HEAD):
        lower = group_index * group_width
        term = jnp.dot(retained[:, lower:lower + group_width], output_retain[:, lower:lower + group_width].T, preferred_element_type=jnp.float32)
        rounded = lax.optimization_barrier(term.astype(jnp.bfloat16))
        mixed = mixed + rounded.astype(jnp.float32)
    decoded = input_full + mixed
    normed_two = row_norm(decoded).astype(jnp.bfloat16)
    key_rows = jnp.dot(normed_two, key_global, preferred_element_type=jnp.float32).astype(jnp.bfloat16)
    value_rows = jnp.dot(normed_two, value_global, preferred_element_type=jnp.float32).astype(jnp.bfloat16)
    cross_queries = (jnp.dot(normed_two, query_cross, preferred_element_type=jnp.float32) * HD ** (-0.5)).astype(jnp.bfloat16)
    group_size = Q_CROSS // KV_HEADS
    key_heads = key_rows.reshape(TOKENS, KV_HEADS, HD).astype(jnp.float32)
    value_heads = value_rows.reshape(TOKENS, KV_HEADS, HD).astype(jnp.float32)
    query_blocks = cross_queries.reshape(N_SEQ, TOK_DEV, KV_HEADS, group_size, HD)
    block_starts = jnp.arange(N_SEQ, dtype=jnp.int32) * TOK_DEV

    def attend(block_items):
        query_block, block_start = block_items
        scores = jnp.einsum('tgqd,sgd->gqts', query_block.astype(jnp.float32), key_heads)
        query_positions = block_start + jnp.arange(TOK_DEV, dtype=jnp.int32)
        allowed = jnp.arange(TOKENS, dtype=jnp.int32)[None, :] <= query_positions[:, None]
        masked = jnp.where(allowed, scores, -1e+30)
        row_top = lax.optimization_barrier(jnp.max(masked, axis=-1, keepdims=True))
        probabilities = jnp.where(allowed, jnp.exp(masked - row_top), 0.0)
        row_total = lax.optimization_barrier(jnp.sum(probabilities, axis=-1))
        rounded = lax.optimization_barrier(probabilities.astype(jnp.bfloat16))
        gathered = jnp.einsum('gqts,sgd->gqtd', rounded.astype(jnp.float32), value_heads)
        result = gathered / row_total[..., None]
        return result.transpose(2, 0, 1, 3).reshape(TOK_DEV, Q_CROSS * HD).astype(jnp.bfloat16)
    attended = lax.map(attend, (query_blocks, block_starts)).reshape(TOKENS, Q_CROSS * HD)
    return (decoded, attended)
```

```python
import functools

import jax
import jax.numpy as jnp
from jax import lax
from jax.experimental import pallas as pl
from jax.experimental.pallas import tpu as pltpu
from jax.sharding import PartitionSpec as P

HD = 128
QUAD = 4
EXACT = 16
LATE = 4
LAG = 3
F32 = jnp.float32
BF16 = jnp.bfloat16
MESH = pl.DeviceIdType.MESH
SPOT = (0, 2, 1, 3)


def dot(a, b, dims=((1,), (0,)), precision=None):
    return lax.dot_general(a, b, (dims, ((), ())), precision=precision, preferred_element_type=F32)


def kernel(n, aligned, *refs):
    it = iter(refs)
    take = lambda k: tuple(next(it) for _ in range(k))
    decay_ref, x_in = take(2)
    (xs_ref,) = (None,) if aligned else take(1)
    w_in = take(7)
    mix_ref, att_ref = take(2)
    wk_ref, wv_ref, wq_ref, wo_ref, wc_ref, wkg_ref, wvg_ref = w_in
    (x_ref,) = take(1)
    gw, go, gkv, gc, xq, tots, states, kvs = take(8)
    run_row_ref, run_col_ref, tot_ref, scale_ref = take(4)
    keep, xs, xr, zs, zr = take(5)
    q_buf, k_buf, v_buf, within_buf, rt = take(5)
    part, got_a, pair, got_b, mix, outm, dn, sq, sq_got = take(9)
    q_rows, top, acc = take(3)
    att_buf, in_sem, out_sem, att_sem = take(4)
    nq, fold, sx, sx_got, xh, xh_got, zh, zh_got = take(8)
    sx_send, sx_recv, xh_send, xh_recv, zh_send, zh_recv = take(6)
    (
        w_send, w_recv, x_send, x_recv, x_local,
        r1_send, r1_recv, r2_send, r2_recv, t_send, t_recv,
        s_send, s_recv, sq_send, sr_send, kv_send, kv_recv, kvq_send, kvr_send,
        a_send, a_recv, h_send, h_recv, q_send, q_recv, o_send, o_recv,
    ) = take(27)

    me = lax.axis_index("seq")
    head = lax.axis_index("head")
    rows, width = x_ref.shape
    depth, inner = wq_ref.shape
    heads = inner // HD
    blocks = n // QUAD
    kd = blocks * depth
    half = kd // 2
    odd = lax.rem(me, 2)
    across = 2 - 4 * lax.rem(me // 2, 2)
    twin = me + 1 - 2 * odd
    partner = (me, twin, me + across, twin + across)
    member = tuple(lax.rem(p, QUAD) for p in partner)
    place = me // QUAD
    inner_place = lax.rem(me // 2, 2) != lax.rem(place, 2)
    core = lax.rem(head, 2)
    near = head + 1 - 2 * core
    far = lax.rem(head + 2, 4)

    def columns(ref):
        return tuple(ref.at[:, h * HD:(h + 1) * HD] for h in range(heads))

    wk, wv, wq = columns(wk_ref), columns(wv_ref), columns(wq_ref)
    own = []
    for h in range(heads):
        own += [wk[h], wv[h]]
    own += wq
    first_out = len(own)
    own += list(columns(wo_ref))
    first_glob = len(own)
    own += [wkg_ref, wvg_ref, *columns(wc_ref)]
    count = len(own)

    def span(i):
        return slice(i * rows, (i + 1) * rows)

    def to_seq(src, dst, send, recv, other):
        return pltpu.make_async_remote_copy(
            src, dst, send, recv, device_id={"seq": other}, device_id_type=MESH)

    def to_head(src, dst, send, recv, other):
        return pltpu.make_async_remote_copy(
            src, dst, send, recv, device_id={"head": other}, device_id_type=MESH)

    def slot(i, o):
        at = pl.ds(pl.multiple_of(o * depth, depth), depth)
        if first_out <= i < first_glob:
            h = i - first_out
            return go.at[at, h * HD:(h + 1) * HD]
        if i < first_out:
            return gw.at[i, at, :]
        g = i - first_glob
        if g < 2:
            return gkv.at[at, g * HD:(g + 1) * HD]
        return gc.at[at, (g - 2) * HD:(g - 1) * HD]

    x_load = pltpu.make_async_copy(x_in, x_ref, in_sem.at[0])
    x_load.start()
    def group(i):
        return 0 if i < first_out else 1 if i < first_glob else 2 if i < first_glob + 2 else 3

    for i in range(count):
        pltpu.make_async_copy(own[i], slot(i, place), in_sem.at[1 + group(i)]).start()

    def whole(ref, sem):
        pltpu.make_async_copy(ref, ref, sem).wait()

    def gone(ref, sem):
        to_seq(ref, ref, sem, x_recv.at[0, 0], twin).wait_send()

    def group_refs(size):
        return (gw.at[:, :size, :], go.at[:size, :], gkv.at[:size, :], gc.at[:size, :])

    barrier = pltpu.get_barrier_semaphore()

    @pl.loop(0, n - 1)
    def _(k):
        pl.semaphore_signal(
            barrier, inc=1, device_id={"seq": lax.rem(me + 1 + k, n)}, device_id_type=MESH
        )

    for other in (near, far):
        pl.semaphore_signal(barrier, inc=1, device_id={"head": other}, device_id_type=MESH)
    pl.semaphore_wait(barrier, n + 1)

    upper = head // 2
    piece = rows // 2

    def x_view(k, ups, side):
        if aligned:
            at = pl.multiple_of((QUAD * side + member[k]) * depth, depth)
            return x_ref.at[ups, pl.ds(at, depth)]
        return xs_ref.at[member[k], ups, pl.ds(pl.multiple_of(side * half, half), half)]

    def some_rows(base, up):
        return pl.ds(pl.multiple_of(base + up * piece, piece), piece)

    def side_cols(side):
        return pl.ds(pl.multiple_of(side * half, half), half)

    def spread(src, dst, send, recv):
        def hop(k):
            return to_seq(src(k), dst(k, upper, core), send.at[0], recv.at[0, k - 1], partner[k])

        def to_far(k):
            ref = dst(k, upper, core)
            return to_head(ref, ref, send.at[0], recv.at[1, k - 1], far)

        def to_near(k):
            ref = dst(k, upper, core)
            return to_head(ref, ref, send.at[0], recv.at[2, k - 1], near)

        def to_near_too(k):
            ref = dst(k, 1 - upper, core)
            return to_head(ref, ref, send.at[0], recv.at[3, k - 1], near)

        def landed(order):
            for k in order:
                hop(k).wait_recv()
                to_far(k).start()
                to_near(k).start()

        def crossed(order):
            for k in order:
                to_far(k).wait_recv()
                to_near_too(k).start()

        def settled(k):
            to_near(k).wait_recv()
            to_near_too(k).wait_recv()

        def sent():
            gone(mix.at[:3], send.at[0])

        return hop, landed, crossed, settled, sent

    x_hop, x_landed, x_crossed, x_settled, x_sent = spread(
        lambda k: x_view(k, some_rows(0, upper), core),
        lambda k, up, side: xq.at[some_rows(SPOT[k] * rows, up), side_cols(side)],
        x_send, x_recv)

    def x_own(side):
        return pltpu.make_async_copy(
            x_view(0, slice(None), side), xq.at[span(0), side * half:(side + 1) * half], x_local.at[0])

    def w_copy(i, k):
        ref = slot(i, place)
        return to_seq(ref, ref, w_send.at[group(i)], w_recv.at[i, k - 1], lax.rem(me + QUAD * k, n))

    def w_from(i, k):
        ref = slot(i, lax.rem(place + blocks - k, blocks))
        return to_seq(ref, ref, w_send.at[group(i)], w_recv.at[i, k - 1], twin)

    def w_start(i):
        @pl.loop(1, blocks)
        def _(k):
            w_copy(i, k).start()

    def w_wait(i):
        @pl.loop(1, blocks)
        def _(k):
            w_from(i, k).wait_recv()

    x_load.wait()
    for k in (2, 3, 1):
        x_hop(k).start()
    for i, ref in enumerate(group_refs(depth)):
        whole(ref, in_sem.at[1 + i])

    def starts(here, which):
        @pl.when(here)
        def _():
            for i in which:
                w_start(i)

    outer_place = jnp.logical_not(inner_place)
    starts(inner_place, range(first_out))
    starts(outer_place, range(LATE))
    for side in range(2):
        x_own(side).start()

    @pl.loop(0, n)
    def _(o):
        kvs[o, :, 2 * HD:] = jnp.ones((rows, HD), BF16)

    t_iota = lax.broadcasted_iota(jnp.int32, (rows, rows), 0)
    s_iota = lax.broadcasted_iota(jnp.int32, (rows, rows), 1)
    run_row_ref[...] = jnp.zeros_like(run_row_ref)
    run_row_ref[:heads, :] = decay_ref[...]
    lower = (s_iota <= t_iota).astype(F32)
    logs = run_row_ref[...]
    run_col_ref[...] = dot(lower, logs, ((1,), (1,)), lax.Precision.HIGHEST)
    run_row_ref[...] = dot(logs, lower, ((1,), (1,)), lax.Precision.HIGHEST)
    tot_ref[...] = jnp.broadcast_to(run_row_ref[:, rows - 1:rows], tot_ref.shape)

    def total_copy(p):
        return to_seq(tot_ref, tots.at[me], t_send.at[p], t_recv.at[me], p)

    @pl.loop(me + 1, n)
    def _(p):
        total_copy(p).start()

    @pl.loop(0, rows // 32)
    def _(i):
        part_rows = pl.ds(i * 32, 32)
        sums_ = jnp.zeros((32, HD), F32)
        for c in range(width // HD):
            x = x_ref[part_rows, c * HD:(c + 1) * HD].astype(F32)
            sums_ = sums_ + x * x
        fold[part_rows, :] = sums_

    ones = jnp.ones((8, HD), F32)
    eye = (s_iota == t_iota).astype(F32)
    sx[...] = dot(ones, fold[...], ((1,), (1,)), lax.Precision.HIGHEST)

    def row_copy(k):
        return to_seq(sx, sx_got.at[k], sx_send.at[0], sx_recv.at[k - 1], partner[k])

    for k in (1, 2, 3):
        row_copy(k).start()

    def scale_of(row):
        column = dot(eye, row, ((1,), (1,)), lax.Precision.HIGHEST)
        return lax.rsqrt(column[:, :1] / width + 1e-06)

    def normalise(k):
        scale_ref[...] = scale_of(sx[...] if k == 0 else sx_got[k])
        start = SPOT[k] * rows

        @pl.loop(0, rows // 32)
        def _(i):
            at = pl.ds(pl.multiple_of(start + i * 32, 32), 32)
            nq[at, :] = (
                xq[at, :].astype(F32) * scale_ref[pl.ds(pl.multiple_of(i * 32, 32), 32), :]
            ).astype(BF16)

    def hop_one(j, part_, first):
        return to_seq(xs.at[j, part_], xr.at[j, part_], r1_send.at[0],
                      r1_recv.at[j, part_], partner[first])

    def hop_two(j, first):
        return to_seq(zs.at[j], zr.at[j], r2_send.at[0], r2_recv.at[j], partner[3 - first])

    def exact_one(j):
        return to_seq(xh.at[j], xh_got.at[j], xh_send.at[0], xh_recv.at[j], partner[1])

    def exact_two(j):
        return to_seq(zh.at[j], zh_got.at[j], zh_send.at[0], zh_recv.at[j], partner[2])

    def rs_put(j, first, k, value):
        if k == first or k == 3:
            xs[j, k // 3] = value.astype(BF16)
            if j < first_out:
                xh[j, k // 3] = value[:EXACT]
        else:
            keep[j, (k + 1) // 2] = value

    def rs_send(j, first, k):
        if k == first or k == 3:
            hop_one(j, k // 3, first).start()

    def rs_begin(j, src):
        weights = gw[j]
        for k in (3, 1):
            rs_put(j, 1, k, dot(src[span(SPOT[k]), :], weights))
        exact_one(j).start()
        for k in (3, 1):
            rs_send(j, 1, k)
        for k in (2, 0):
            rs_put(j, 1, k, dot(src[span(SPOT[k]), :], weights))

    def rs_mid(j, first):
        hop_one(j, 1, first).wait_recv()
        zs[j] = (keep[j, 1] + xr[j, 1].astype(F32)).astype(BF16)
        hop_two(j, first).start()
        if j < first_out:
            exact_one(j).wait_recv()
            zh[j] = keep[j, 1, :EXACT] + xh_got[j, 1]
            exact_two(j).start()

    def rs_end(j, first):
        hop_one(j, 0, first).wait_recv()
        hop_two(j, first).wait_recv()
        value = keep[j, 0] + xr[j, 0].astype(F32) + zr[j].astype(F32)
        if j < first_out:
            exact_two(j).wait_recv()
            exact = keep[j, 0, :EXACT] + xh_got[j, 0] + zh_got[j]
            value = jnp.concatenate([exact, value[EXACT:]], axis=0)
        return value

    top_pair = lax.rem(me // 2, 2) == 1

    def causal_ops(view, send, recv, quad_send, relay_send):
        def later(k):
            return to_seq(view(me), view(me), send(k), recv(me), me + QUAD * k)

        def near_by(k):
            return to_seq(view(me), view(me), quad_send(k), recv(me), partner[k])

        def pass_on(k, j):
            o = me - QUAD * j
            return to_seq(view(o), view(o), relay_send(k, j), recv(o), partner[k])

        def second(j):
            o = partner[2] - QUAD * j
            sem = quad_send(3) if isinstance(j, int) else relay_send(3, j)
            return to_seq(view(o), view(o), sem, recv(o), twin)

        def land(o):
            to_seq(view(o), view(o), quad_send(1), recv(o), twin).wait_recv()

        def earlier(body):
            pl.loop(1, place + 1)(body)

        def start_far():
            @pl.loop(1, blocks - place)
            def _(k):
                later(k).start()

        def start():
            for k in (2, 1):
                @pl.when(partner[k] > me)
                def _():
                    near_by(k).start()

        def relay():
            @earlier
            def _(j):
                land(me - QUAD * j)
                for k in (2, 1):
                    pass_on(k, j).start()

        def relay_two():
            @pl.when(top_pair)
            def _():
                land(partner[2])
                second(0).start()

            @earlier
            def _(j):
                land(partner[2] - QUAD * j)
                second(j).start()

        def finish(use=lambda o: None):
            @earlier
            def _(j):
                use(me - QUAD * j)
                use(partner[2] - QUAD * j)

            @pl.when(top_pair)
            def _():
                use(partner[2])

            @pl.when(odd == 1)
            def _():
                land(twin)
                use(twin)

            @earlier
            def _(j):
                land(twin - QUAD * j)
                use(twin - QUAD * j)

        def finish_far(use=lambda o: None):
            @pl.when(top_pair)
            def _():
                land(partner[3])
                use(partner[3])

            @earlier
            def _(j):
                land(partner[3] - QUAD * j)
                use(partner[3] - QUAD * j)

        def finish_sends():
            @pl.loop(1, blocks - place)
            def _(k):
                later(k).wait_send()

            for k in (2, 1):
                @pl.when(partner[k] > me)
                def _():
                    near_by(k).wait_send()

            @pl.when(top_pair)
            def _():
                second(0).wait_send()

            @earlier
            def _(j):
                for k in (2, 1):
                    pass_on(k, j).wait_send()
                second(j).wait_send()

        return start_far, start, relay, relay_two, finish, finish_far, finish_sends

    state_ops = [
        causal_ops(
            lambda o, h=h: states.at[o, h * HD:(h + 1) * HD, :],
            lambda k, h=h: s_send.at[h, k - 1],
            lambda o, h=h: s_recv.at[h, o],
            lambda k, h=h: sq_send.at[h, k - 1],
            lambda k, j, h=h: sr_send.at[h, k - 1, j - 1],
        )
        for h in range(heads)
    ]

    def ret_copy(h, k):
        cols = slice(h * HD, (h + 1) * HD)
        return to_seq(rt.at[span(0), cols], rt.at[span(SPOT[k]), cols],
                      a_send.at[0], a_recv.at[h, k - 1], partner[k])

    def ret_relay(h):
        cols = slice(h * HD, (h + 1) * HD)
        return to_seq(rt.at[span(SPOT[2]), cols], rt.at[span(SPOT[3]), cols],
                      a_send.at[0], a_recv.at[h, 2], twin)

    def send_state(h):
        cols = slice(h * HD, (h + 1) * HD)
        tail = jnp.exp(run_row_ref[h:h + 1, rows - 1:rows] - run_col_ref[:, h:h + 1])
        faded = (k_buf[:, cols].astype(F32) * tail).astype(BF16)
        states[me, cols, :] = dot(faded, v_buf[:, cols], ((0,), (0,))).astype(BF16)
        state_ops[h][0]()
        state_ops[h][1]()

    def within(h):
        cols = slice(h * HD, (h + 1) * HD)
        causal = t_iota >= s_iota
        spread = jnp.where(causal, run_col_ref[:, h:h + 1] - run_row_ref[h:h + 1, :], 0.0)
        decay = jnp.where(causal, jnp.exp(spread), 0.0)
        scores = dot(q_buf[:, cols], k_buf[:, cols], ((1,), (1,)))
        weighted = (scores * decay).astype(BF16)
        within_buf[:, cols] = dot(weighted, v_buf[:, cols])

    def retain(h):
        cols = slice(h * HD, (h + 1) * HD)
        state_ops[h][4]()
        state_ops[h][5]()

        def step(o, state):
            return jnp.exp(tots[o, h:h + 1, :]) * state + states[o, cols, :].astype(F32)

        incoming = lax.fori_loop(0, me, step, jnp.zeros((HD, HD), F32))
        carried = dot(
            q_buf[:, cols].astype(F32), incoming, precision=lax.Precision.HIGHEST
        ) * jnp.exp(run_col_ref[:, h:h + 1])
        raw = within_buf[:, cols] + carried
        rt[span(0), cols] = (
            raw * lax.rsqrt(jnp.mean(raw * raw, axis=-1, keepdims=True) + 1e-06)).astype(BF16)
        ret_copy(h, 2).start()
        ret_copy(h, 1).start()

    x_landed((1, 2, 3))
    x_crossed((1, 2, 3))
    whole(xq.at[span(0), :], x_local.at[0])
    normalise(0)
    for k in (1, 2, 3):
        x_settled(k)
        row_copy(k).wait_recv()
        normalise(k)

    for i in range(first_out + LAG):
        if i < first_out:
            w_wait(i)
            if i + LATE < first_out:
                starts(outer_place, (i + LATE,))
            rs_begin(i, nq)
        if 1 <= i <= first_out:
            rs_mid(i - 1, 1)
        if i == first_out:
            for m in range(first_out, first_glob):
                w_start(m)
            for h in range(heads):
                state_ops[h][2]()
        if i == first_out + 1:
            for h in range(heads):
                state_ops[h][3]()
        if i < LAG:
            continue
        j = i - LAG
        value = rs_end(j, 1).astype(BF16)
        h, m = (j - 2 * heads, 2) if j >= 2 * heads else divmod(j, 2)
        (k_buf, v_buf, q_buf)[m][:, h * HD:(h + 1) * HD] = value
        if m == 1:
            send_state(h)
        if m == 2:
            within(h)

    @pl.loop(0, me)
    def _(o):
        to_seq(tots.at[o], tots.at[o], t_send.at[o], t_recv.at[o], twin).wait_recv()

    for h in range(heads):
        retain(h)
    w_start(first_glob)
    w_start(first_glob + 1)

    def near_copy(s):
        return to_head(part.at[s, 1 - core], got_a.at[s], h_send.at[0], h_recv.at[0, s], near)

    def far_copy(s):
        return to_head(pair.at[s], got_b.at[s], h_send.at[1], h_recv.at[1, s], far)

    def back_copy(s):
        ref = mix.at[s, core]
        return to_head(ref, ref, h_send.at[2], h_recv.at[2, s], near)

    for i in range(first_out, first_glob):
        w_wait(i)

    def project(s, side):
        part[s, side] = dot(
            rt[span(s), :], go[pl.ds(pl.multiple_of(side * half, half), half), :], ((1,), (1,))
        ).astype(BF16)

    def combine(s):
        near_copy(s).wait_recv()
        pair[s] = (part[s, core].astype(F32) + got_a[s].astype(F32)).astype(BF16)
        far_copy(s).start()

    trip = (SPOT[0], SPOT[1], SPOT[3], SPOT[2])
    for s in trip:
        if s == SPOT[1]:
            for h in range(heads):
                ret_copy(h, 2).wait_recv()
                ret_relay(h).start()
            for h in range(heads):
                ret_copy(h, 1).wait_recv()
        if s == SPOT[3]:
            for i in range(first_glob + 2, count):
                w_start(i)
            for h in range(heads):
                ret_relay(h).wait_recv()
        project(s, 1 - core)
        near_copy(s).start()
        project(s, core)
        combine(s)

    def square_copy(k):
        return to_seq(sq.at[SPOT[k]], sq_got.at[k], q_send.at[0], q_recv.at[k - 1], partner[k])

    out_hop, out_landed, out_crossed, out_settled, out_sent = spread(
        lambda k: mix.at[SPOT[k], core, some_rows(0, upper), :],
        lambda k, up, side: outm.at[k, side, some_rows(0, up), :],
        o_send, o_recv)

    kv_ops = causal_ops(
        lambda o: kvs.at[o, :, :2 * HD], lambda k: kv_send.at[k - 1], lambda o: kv_recv.at[o],
        lambda k: kvq_send.at[k - 1], lambda k, j: kvr_send.at[k - 1, j - 1])

    base = first_out
    def kv_part(k):
        value = dot(dn[span(SPOT[k]), :], gkv[...])
        for g in range(2):
            rs_put(base + g, 1, k, value[:, g * HD:(g + 1) * HD])
        for g in range(2):
            rs_send(base + g, 1, k)

    def kv_end(g):
        return (rs_end(base + g, 1) * scale_ref[...]).astype(BF16)

    turn = [1, 1] + [1 + g % 2 for g in range(heads)]

    def cross_part(k):
        value = dot(dn[span(SPOT[k]), :], gc[...])
        for g in crosses:
            rs_put(base + g, turn[g], k, value[:, (g - 2) * HD:(g - 1) * HD])
        for g in crosses:
            rs_send(base + g, turn[g], k)

    def cross_end(g):
        return rs_end(base + g, turn[g]) * scale_ref[...]

    crosses = tuple(range(2, 2 + heads))
    w_wait(first_glob)
    w_wait(first_glob + 1)
    for t, s in enumerate(trip):
        k = SPOT.index(s)
        far_copy(s).wait_recv()
        mix[s, core] = (pair[s].astype(F32) + got_b[s].astype(F32)).astype(BF16)
        back_copy(s).start()
        back_copy(s).wait_recv()
        squares = jnp.zeros((rows, HD), F32)
        for side in range(2):
            cols = slice(side * half, (side + 1) * half)
            d = xq[span(s), cols].astype(F32) + mix[s, side].astype(F32)
            dn[span(s), cols] = d.astype(BF16)
            for c in range(half // HD):
                lanes = d[:, c * HD:(c + 1) * HD]
                squares = squares + lanes * lanes
        kv_part(k)
        sq[s] = dot(ones, squares, ((1,), (1,)), lax.Precision.HIGHEST)
        if k:
            square_copy(k).start()
        if t == 2:
            out_hop(1).start()
            out_hop(3).start()
    rs_mid(base, 1)
    rs_mid(base + 1, 1)
    out_hop(2).start()
    for g in crosses:
        w_wait(first_glob + g)
    for k in (3, 1, 2, 0):
        cross_part(k)
    for k in (1, 2, 3):
        square_copy(k).wait_recv()
    squares = sq[0] + sq_got[1] + sq_got[2] + sq_got[3]
    scale_ref[...] = scale_of(squares)
    kvs[me, :, :HD] = kv_end(0)
    kvs[me, :, HD:2 * HD] = kv_end(1)
    kv_ops[0]()
    for g in crosses:
        rs_mid(base + g, turn[g])
    kv_ops[1]()
    out_landed((1, 3, 2))
    kv_ops[2]()
    for g in range(heads):
        block = span(g)
        q_rows[block, :] = (cross_end(2 + g) * HD ** -0.5).astype(BF16)
        scores = dot(q_rows[block, :], kvs[me, :, :HD], ((1,), (1,)))
        scores = jnp.where(t_iota >= s_iota, scores, -1e30)
        high = jnp.max(scores, axis=-1, keepdims=True)
        weights = jnp.exp(scores - high)
        top[block, :] = jnp.broadcast_to(high, (rows, HD))
        acc[block, :] = dot(weights.astype(BF16), kvs[me, :, HD:])
    kv_ops[3]()

    def attend(o):
        for g in range(heads):
            block = span(g)
            scores = dot(q_rows[block, :], kvs[o, :, :HD], ((1,), (1,)))
            old = top[block, :]
            high = jnp.maximum(old, jnp.max(scores, axis=-1, keepdims=True))
            weights = jnp.concatenate(
                [jnp.exp(scores[:, c:c + HD] - high) for c in range(0, rows, HD)], axis=1)
            shrink = jnp.exp(old - high)
            top[block, :] = high
            fresh = dot(weights.astype(BF16), kvs[o, :, HD:])
            for c in range(0, 2 * HD, HD):
                acc[block, c:c + HD] = acc[block, c:c + HD] * shrink + fresh[:, c:c + HD]

    def put(k, side):
        if aligned:
            at = pl.multiple_of((QUAD * side + member[k]) * depth, depth)
            dst = mix_ref.at[:, pl.ds(at, depth)]
        else:
            dst = mix_ref.at[member[k], :, side * half:(side + 1) * half]
        src = mix.at[0, side] if k == 0 else outm.at[k, side]
        return pltpu.make_async_copy(src, dst, out_sem.at[0])

    for side in range(2):
        put(0, side).start()
    kv_ops[4](attend)
    out_crossed((1, 3, 2))
    kv_ops[5](attend)
    for k in (2, 1, 3):
        out_settled(k)
        for side in range(2):
            put(k, side).start()

    def att_copy(g):
        cols = slice(g * HD, (g + 1) * HD)
        return pltpu.make_async_copy(att_buf.at[:, cols], att_ref.at[:, cols], att_sem.at[0])

    for g in range(heads):
        block = span(g)
        att_buf[:, g * HD:(g + 1) * HD] = (acc[block, :HD] / acc[block, HD:]).astype(BF16)
        att_copy(g).start()

    @pl.loop(me + 1, n)
    def _(p):
        total_copy(p).wait_send()

    for i, ref in enumerate(group_refs(kd - depth)):
        gone(ref, w_send.at[i])
    x_sent()
    out_sent()
    gone(xs, r1_send.at[0])
    gone(zs, r2_send.at[0])
    gone(sx_got.at[1:], sx_send.at[0])
    gone(xh, xh_send.at[0])
    gone(zh, zh_send.at[0])
    gone(sq.at[1:], q_send.at[0])
    gone(rt.at[rows:, :], a_send.at[0])
    for i in range(3):
        gone(pair, h_send.at[i])
    for h in range(heads):
        state_ops[h][6]()
    kv_ops[6]()
    whole(mix_ref, out_sem.at[0])
    whole(att_ref, att_sem.at[0])


def body(n, inputs, decay_logs, wq, wk, wv, wo, kg, vg, qc):
    rows, width = inputs.shape
    depth, inner = wq.shape
    heads = inner // HD
    blocks = n // QUAD
    kd = blocks * depth
    half = kd // 2
    aligned = depth % HD == 0 and blocks == 2
    vmem = pl.BlockSpec(memory_space=pltpu.VMEM)
    dma = pltpu.SemaphoreType.DMA
    sums = 4 * heads + 2
    count = 5 * heads + 2

    def bf(*shape):
        return pltpu.VMEM(shape, BF16)

    def f32(*shape):
        return pltpu.VMEM(shape, F32)

    args = [decay_logs, inputs]
    if not aligned:
        args.append(
            inputs.reshape(rows, blocks, QUAD, depth).transpose(2, 0, 1, 3).reshape(QUAD, rows, kd))
    args += [wk, wv, wq, wo, qc, kg, vg]
    anywhere = pl.BlockSpec(memory_space=pl.ANY)
    specs = [vmem, anywhere] + [vmem] * (not aligned) + [anywhere] * 7
    mixed_shape = (rows, width) if aligned else (QUAD, rows, kd)
    mixed, attended = pl.pallas_call(
        functools.partial(kernel, n, aligned),
        out_shape=(
            jax.ShapeDtypeStruct(mixed_shape, BF16),
            jax.ShapeDtypeStruct((rows, inner), BF16),
        ),
        in_specs=specs,
        out_specs=(anywhere, anywhere),
        scratch_shapes=[
            bf(rows, width),
            bf(3 * heads, kd, HD), bf(kd, inner), bf(kd, 2 * HD), bf(kd, inner), bf(QUAD * rows, kd),
            f32(n, 8, HD), bf(n, inner, HD), bf(n, rows, 3 * HD),
            f32(8, rows), f32(rows, 8), f32(8, HD), f32(rows, 1),
            f32(sums, 2, rows, HD), bf(sums, 2, rows, HD), bf(sums, 2, rows, HD),
            bf(sums, rows, HD), bf(sums, rows, HD),
            bf(rows, inner), bf(rows, inner), bf(rows, inner), f32(rows, inner),
            bf(QUAD * rows, inner),
            bf(QUAD, 2, rows, half), bf(QUAD, rows, half), bf(QUAD, rows, half),
            bf(QUAD, rows, half), bf(QUAD, 2, rows, half), bf(QUAD, 2, rows, half),
            bf(QUAD * rows, kd), f32(QUAD, 8, rows), f32(QUAD, 8, rows),
            bf(heads * rows, HD), f32(heads * rows, HD),
            f32(heads * rows, 2 * HD),
            bf(rows, inner), dma((5,)), dma((1,)), dma((1,)),
            bf(QUAD * rows, kd), f32(rows, HD), f32(8, rows), f32(QUAD, 8, rows),
            f32(3 * heads, 2, EXACT, HD), f32(3 * heads, 2, EXACT, HD),
            f32(3 * heads, EXACT, HD), f32(3 * heads, EXACT, HD),
            dma((1,)), dma((3,)), dma((1,)), dma((3 * heads,)), dma((1,)), dma((3 * heads,)),
            dma((4,)), dma((count, blocks - 1)),
            dma((1,)), dma((4, 3)), dma((1,)),
            dma((1,)), dma((sums, 2)), dma((1,)), dma((sums,)), dma((n,)), dma((n,)),
            dma((heads, blocks - 1)), dma((heads, n)), dma((heads, 3)), dma((heads, 3, blocks - 1)),
            dma((blocks - 1,)), dma((n,)), dma((3,)), dma((3, blocks - 1)),
            dma((1,)), dma((heads, 3)), dma((3,)), dma((3, QUAD)),
            dma((1,)), dma((3,)), dma((1,)), dma((4, 3)),
        ],
        compiler_params=pltpu.CompilerParams(
            collective_id=0, has_side_effects=True, vmem_limit_bytes=62 * 1024 * 1024),
        name="layer",
    )(*args)
    if not aligned:
        mixed = mixed.reshape(QUAD, rows, blocks, depth).transpose(1, 2, 0, 3).reshape(rows, width)
    return finish_rows(inputs, mixed, attended)


def finish_kernel(x_ref, mix_ref, att_in, dec_ref, att_ref):
    dec_ref[...] = x_ref[...].astype(F32) + mix_ref[...].astype(F32)
    att_ref[...] = att_in[...]


def finish_rows(inputs, mixed, attended):
    rows, width = inputs.shape
    inner = attended.shape[1]
    steps = 4
    wide = pl.BlockSpec((rows // steps, width), lambda i: (i, 0))
    thin = pl.BlockSpec((rows // steps, inner), lambda i: (i, 0))
    return pl.pallas_call(
        finish_kernel,
        grid=(steps,),
        out_shape=(
            jax.ShapeDtypeStruct((rows, width), F32),
            jax.ShapeDtypeStruct((rows, inner), BF16),
        ),
        in_specs=[wide, wide, thin],
        out_specs=(wide, thin),
        name="finish",
    )(inputs, mixed, attended)


def solution(mesh):
    n = mesh.shape["seq"]

    def run(*args):
        return body(n, *args)

    in_specs = (P("seq", None), P("head", "seq")) + (P("seq", "head"),) * 7
    out_specs = (P("seq", None), P("seq", "head"))
    return jax.shard_map(run, mesh=mesh, in_specs=in_specs, out_specs=out_specs, check_vma=False)
```
